256 devices in a mesh: gy: 16 (over x_hi, y, core), gx: 16 (over x_lo, z).
Axes of the slice: x: 4 (x_hi: 2, x_lo: 2; x = x_hi * 2 + x_lo), y: 4, z: 8, core: 2. Of those that a mesh axis runs over, the one named last changes fastest.
Arguments:
- feat_a: float32 [1024, 1024, 128], P('gy', 'gx'), may hold values from -8 to 8
- feat_b: float32 [1024, 1024, 128], P('gy', 'gx'), may hold values from -8 to 8
- occ_a: int32 [1024, 1024], P('gy', 'gx'), may hold values from 0 to 1, as said below
- occ_b: int32 [1024, 1024], P('gy', 'gx'), may hold values from 0 to 1, as said below
- first_weight: bfloat16 [256, 256], replicated, may hold values from -0.375 to 0.375
- second_weight: bfloat16 [256, 128], replicated, may hold values from -0.375 to 0.375
Outputs:
- matched_a: float32 [1024, 1024, 128], P('gy', 'gx')
- matched_b: float32 [1024, 1024, 128], P('gy', 'gx')
The draws below stay inside these ranges and needn't reach their ends.
Inputs may be any that keep to these rules, and one draw needn't show every extreme that they name: `occ_a`: 1 marks an occupied cell. `occ_b`: 1 marks an occupied cell.
All inputs are finite; a program needn't handle non-finite values.
Results may differ from the reference program's by a relative error of at most 0.0042.
Values may be sent and summed in bfloat16 or wider, within the bound.
No kernel may reach another device: no remote copies, remote signals or barrier semaphores. Data moves between devices by JAX's collectives and lax.ppermute only.
A program may use at most 64 MiB of HBM per device.

```python
import jax
import jax.numpy as jnp
from jax import lax

C = 128
H = 256
R = 8
NY = 1024
NX = 1024


def feature_pair(key):
    keys_list = jax.random.split(jax.random.fold_in(key, 7101), 5)
    first = jax.random.normal(keys_list[3], (NY, NX, C), jnp.float32)
    second = jax.random.normal(keys_list[4], (NY, NX, C), jnp.float32)
    return (jnp.clip(first, -8.0, 8.0), jnp.clip(second, -8.0, 8.0))


def draw_feat_a(key, part):
    return feature_pair(key)[0]


def draw_feat_b(key, part):
    return feature_pair(key)[1]


def occupied_cells(key):
    keys_list = jax.random.split(key, 3)
    patch_level = jax.random.randint(keys_list[0], (NY // 8 + 1, NX // 32 + 1), 0, 4)
    region_level = jax.random.randint(keys_list[1], (NY // 64 + 1, NX // 256 + 1), 1, 4)
    row_iota = jnp.arange(NY, dtype=jnp.int32)
    col_iota = jnp.arange(NX, dtype=jnp.int32)
    patches = patch_level[row_iota // 8][:, col_iota // 32]
    regions = region_level[row_iota // 64][:, col_iota // 256]
    threshold = patches * regions * 11
    rolled = jax.random.randint(keys_list[2], (NY, NX), 0, 100)
    return (rolled < threshold).astype(jnp.int32)


def draw_occ_a(key, part):
    return occupied_cells(jax.random.fold_in(key, 5201))


def draw_occ_b(key, part):
    return occupied_cells(jax.random.fold_in(key, 5202))


def normal_values(key, extent, deviation, reach, held_as=jnp.bfloat16):
    return jnp.clip(deviation * jax.random.normal(key, extent, jnp.float32), -reach, reach).astype(held_as)


def setup_inputs(seed: int = 0) -> dict:
    key_of = jax.random.split(jax.random.key(seed), 7)
    feat_a = draw_feat_a(jax.random.fold_in(key_of[6], 71), 0)
    feat_b = draw_feat_b(jax.random.fold_in(key_of[6], 71), 0)
    occ_a = draw_occ_a(jax.random.fold_in(key_of[6], 71), 0)
    occ_b = draw_occ_b(jax.random.fold_in(key_of[6], 71), 0)
    first_weight = normal_values(key_of[4], (2 * C, H), (2 * C) ** -0.5, 0.375)
    second_weight = normal_values(key_of[5], (H, C), H ** -0.5, 0.375)
    return dict(feat_a=feat_a, feat_b=feat_b, occ_a=occ_a, occ_b=occ_b, first_weight=first_weight, second_weight=second_weight)


def transport(queries, keys, key_mask):
    window = 2 * R + 1
    scaling = 1.0 / (C ** 0.5)
    query_full = queries.astype(jnp.float32)
    key_padded = jnp.pad(keys.astype(jnp.float32), ((R, R), (R, R), (0, 0)))
    mask_padded = jnp.pad(key_mask.astype(jnp.float32), ((R, R), (R, R)))
    offsets = jnp.arange(window * window, dtype=jnp.int32)

    def one_band(band_index):
        top_row = band_index * 8
        query_band = lax.dynamic_slice(query_full, (top_row, jnp.int32(0), jnp.int32(0)), (8, NX, C))

        def key_at(offset):
            down_step = offset // window
            across = offset % window
            key_band = lax.dynamic_slice(key_padded, (top_row + down_step, across, jnp.int32(0)), (8, NX, C))
            mask_band = lax.dynamic_slice(mask_padded, (top_row + down_step, across), (8, NX))
            return key_band, mask_band

        def score_at(offset):
            key_band, mask_band = key_at(offset)
            return jnp.sum(query_band * key_band, axis=-1) * scaling, mask_band

        cost_stack, mask_stack = lax.map(score_at, offsets)
        usable = mask_stack > 0
        highest = jnp.max(jnp.where(usable, cost_stack, 0.0), axis=0)
        exponent = jnp.where(usable, jnp.exp(cost_stack - highest), 0.0)
        denominator = jnp.exp(-highest) + jnp.sum(exponent, axis=0)
        weights = lax.optimization_barrier((exponent / denominator).astype(jnp.bfloat16)).astype(jnp.float32)

        def accumulate(carried, element):
            offset, weight = element
            key_band, unused = key_at(offset)
            return carried + weight[..., None] * key_band, None

        gathered, unused = lax.scan(accumulate, jnp.zeros((8, NX, C), jnp.float32), (offsets, weights))
        return gathered

    band_list = lax.map(one_band, jnp.arange(NY // 8, dtype=jnp.int32))
    return band_list.reshape(NY, NX, C)


def refine(feature, half, carried, cell_mask, first_weight, second_weight):
    joined = jnp.concatenate([half, carried.astype(jnp.bfloat16)], axis=-1).reshape(-1, 2 * C)
    hidden = jax.nn.gelu(jnp.dot(joined, first_weight, preferred_element_type=jnp.float32), approximate=False).astype(jnp.bfloat16)
    update = jnp.dot(hidden, second_weight, preferred_element_type=jnp.float32).reshape(feature.shape)
    return feature + cell_mask.astype(jnp.float32)[..., None] * update


def reference(feat_a, feat_b, occ_a, occ_b, first_weight, second_weight):
    for repeat in range(2):
        half_a = feat_a.astype(jnp.bfloat16)
        half_b = feat_b.astype(jnp.bfloat16)
        carried_a = transport(half_a, half_b, occ_b)
        carried_b = transport(half_b, half_a, occ_a)
        feat_a = refine(feat_a, half_a, carried_a, occ_a, first_weight, second_weight)
        feat_b = refine(feat_b, half_b, carried_b, occ_b, first_weight, second_weight)
    return feat_a, feat_b
```

```python
import functools

import jax
import jax.numpy as jnp
from jax import lax
from jax.experimental import pallas as pl
from jax.experimental.pallas import tpu as pltpu
from jax.sharding import PartitionSpec as P

R = 8
T = 16
SENT = 2.0**120
LIMIT = 2.0**110
BIG = 2.0**100
LOG2E = 1.4426950408889634
RSQRT2 = 0.7071067811865476


def key_bias(first_row, col_group):
    cell = lax.broadcasted_iota(jnp.int32, (128, 128), 0)
    lane = lax.broadcasted_iota(jnp.int32, (128, 128), 1)
    row = first_row + cell // T
    col = col_group * T + cell % T
    place = jnp.where(lane < 32, row, col)
    inside = ((place - lane) & 31) <= 2 * R
    return jnp.where((lane >= 64) | inside, 0.0, -BIG)


def query_code(ty, tx):
    cell = lax.broadcasted_iota(jnp.int32, (256, 128), 0)
    lane = lax.broadcasted_iota(jnp.int32, (256, 128), 1)
    row = (ty * T + cell // T) & 31
    col = (tx * T + cell % T) & 31
    hit = (lane == row) | (lane == col + 32) | (lane == 64)
    return jnp.where(hit, 1.0, 0.0).astype(jnp.bfloat16)


def assemble(centers, top, bottom, left, right, kc, ke, vt, pc):
    for s in range(2):

        def group(rg, row_of):
            for r in range(8):
                row = rg * 8 + r
                line = jnp.concatenate(
                    [left[s, row], row_of(row, r), right[s, row]], axis=0
                )
                for cg in range(5):
                    kc[s, rg, cg, r * T : (r + 1) * T, :] = line[cg * T : (cg + 1) * T]
            for cg in range(5):
                raw = kc[s, rg, cg].astype(jnp.float32)
                free = raw > LIMIT
                clean = jnp.where(free, 0.0, raw).astype(jnp.bfloat16)
                kc[s, rg, cg] = clean
                vt[s, rg, cg] = clean.T
                ke[s, rg, cg] = jnp.where(free, -BIG, key_bias(rg * 8, cg)).astype(
                    jnp.bfloat16
                )

        group(0, lambda row, r: top[s, r])
        group(9, lambda row, r: bottom[s, r])

        def step(rg, carry):
            group(rg, lambda row, r: centers[s][row - 8])
            return carry

        lax.fori_loop(1, 9, step, 0)
        for h in range(2):
            n = 768 * (1 - h)
            pc[s, n : n + 256, h * 128 : h * 128 + 128] = jnp.zeros((256, 128), jnp.bfloat16)


def kernel(emit, tiles, ca, cb, top, bottom, left, right, fa, fb, w1, w2, *rest):
    keyed = (None, None)
    if emit:
        oa, ob, *rest = rest
        keyed = (rest[0], rest[1])
        rest = rest[2:]
    else:
        oa, ob, *rest = rest
    kc, ke, vt, sc, pc, ct, mx, sm = rest
    centers = (ca, cb)
    feats = (fa, fb)
    outs = (oa, ob)
    across = tiles[1]
    last = tiles[0] * tiles[1] - 1
    scale = LOG2E / 128.0**0.5
    j = pl.program_id(0)

    def place(t):
        t = jnp.clip(t, 0, last)
        return t // across, t % across

    def tile_of(s, ty, tx):
        raw = centers[s][pl.ds(ty * T, T), pl.ds(pl.multiple_of(tx * T, T), T), :]
        raw = raw.reshape(256, 128).astype(jnp.float32)
        free = raw > LIMIT
        return free, jnp.where(free, 0.0, raw).astype(jnp.bfloat16)

    def score(s, t):
        ty, tx = place(t)
        k = 1 - s
        unused, query = tile_of(s, ty, tx)
        full = jnp.concatenate([query, query_code(ty, tx)], axis=1)
        best = [None, None]
        for i in range(2):
            rows = pl.ds(2 * ty + 2 * i, 2)
            cols = pl.ds(tx, 2)
            keys = jnp.concatenate(
                [
                    kc[k, rows, cols].reshape(512, 128),
                    ke[k, rows, cols].reshape(512, 128),
                ],
                axis=1,
            )
            scores = lax.dot_general(
                keys, full, (((1,), (1,)), ((), ())), preferred_element_type=jnp.float32
            )
            for h in range(2):
                lo, hi = max(256 * h, 512 * i), min(256 * h + 768, 512 * i + 512)
                part = scores[lo - 512 * i : hi - 512 * i, h * 128 : h * 128 + 128]
                sc[s, lo:hi, h * 128 : h * 128 + 128] = part
                top_now = part.reshape((hi - lo) // 8, 8, 128).max(0)
                best[h] = top_now if best[h] is None else jnp.maximum(best[h], top_now)
            yield
        for h in range(2):
            mx[s, :, h * 128 : h * 128 + 128] = best[h]
        yield

    def weigh(s):
        for h in range(2):
            lanes = slice(h * 128, h * 128 + 128)
            best = jnp.maximum(mx[s, :, lanes].max(0, keepdims=True), 0.0)
            total = jnp.zeros((8, 128), jnp.float32)
            for n in range(256 * h, 256 * h + 768, 128):
                e = jnp.exp2((sc[s, n : n + 128, lanes] - best) * scale)
                total = total + e.reshape(16, 8, 128).sum(0)
                pc[s, n : n + 128, lanes] = e.astype(jnp.bfloat16)
                if (n - 256 * h) % 256 == 128:
                    yield
            total = total.sum(0, keepdims=True) + jnp.exp2(-best * scale)
            sm[s, :, lanes] = jnp.broadcast_to(1.0 / total, (8, 128))
        yield

    def gather(s, t):
        ty, tx = place(t)
        k = 1 - s
        values = jnp.concatenate(
            [vt[k, 2 * ty + i, tx + c] for i in range(4) for c in range(2)], axis=1
        )
        carried = jnp.dot(values, pc[s], preferred_element_type=jnp.float32)
        ct[s] = (carried * sm[s][:1]).astype(jnp.bfloat16)
        yield

    def update(s, t):
        ty, tx = place(t)
        free, query = tile_of(s, ty, tx)
        joined = jnp.concatenate([query, ct[s].T], axis=1)
        x = jnp.dot(joined, w1[...], preferred_element_type=jnp.float32)
        hidden = (0.5 * x * (1.0 + lax.erf(x * RSQRT2))).astype(jnp.bfloat16)
        yield
        change = jnp.dot(hidden, w2[...], preferred_element_type=jnp.float32)
        old = feats[s][...].reshape(256, 128)
        new = jnp.where(free, old, old + change)
        outs[s][...] = new.reshape(T, T, 128)
        if emit:
            keyed[s][...] = jnp.where(free, SENT, new).astype(jnp.bfloat16).reshape(T, T, 128)
        yield

    @pl.when(j == 0)
    def _():
        assemble(centers, top, bottom, left, right, kc, ke, vt, pc)
        for unused in score(0, 0):
            pass

    for stages in (
        (update(1, j - 2), gather(1, j - 1), score(1, j), weigh(0)),
        (update(0, j - 1), gather(0, j), score(0, j + 1), weigh(1)),
    ):
        stages = list(stages)
        while stages:
            stages = [stage for stage in stages if next(stage, True) is None]


def one_pass(emit, centers, rims, feat_a, feat_b, first_weight, second_weight):
    rows, cols, channels = feat_a.shape
    tiles = (rows // T, cols // T)
    count = tiles[0] * tiles[1]
    whole = pl.BlockSpec(memory_space=pltpu.VMEM)

    def tile(delay):
        def at(j):
            t = jnp.clip(j - delay, 0, count - 1)
            return t // tiles[1], t % tiles[1], 0

        return pl.BlockSpec((T, T, channels), at)

    out_shape = [jax.ShapeDtypeStruct(feat_a.shape, jnp.float32)] * 2
    out_specs = [tile(1), tile(2)]
    if emit:
        out_shape += [jax.ShapeDtypeStruct(feat_a.shape, jnp.bfloat16)] * 2
        out_specs += [tile(1), tile(2)]
    blocks = (2, (rows + 2 * R) // 8, (cols + 2 * R) // T, 128, 128)
    flops = 2 * 16 * (2 * 1024 * 256 * 256 * 2 + 256 * 256 * 384 * 2)
    return pl.pallas_call(
        functools.partial(kernel, emit, tiles),
        grid=(count + 2,),
        in_specs=[whole] * 6 + [tile(1), tile(2), whole, whole],
        out_specs=out_specs,
        out_shape=out_shape,
        scratch_shapes=[
            pltpu.VMEM(blocks, jnp.bfloat16),
            pltpu.VMEM(blocks, jnp.bfloat16),
            pltpu.VMEM(blocks, jnp.bfloat16),
            pltpu.VMEM((2, 1024, 256), jnp.float32),
            pltpu.VMEM((2, 1024, 256), jnp.bfloat16),
            pltpu.VMEM((2, 128, 256), jnp.bfloat16),
            pltpu.VMEM((2, 8, 256), jnp.float32),
            pltpu.VMEM((2, 8, 256), jnp.float32),
        ],
        compiler_params=pltpu.CompilerParams(
            dimension_semantics=("arbitrary",), vmem_limit_bytes=44 << 20
        ),
        cost_estimate=pl.CostEstimate(
            flops=flops, bytes_accessed=14 << 20, transcendentals=2 * 16 * 768 * 256
        ),
        name="match_pass",
    )(*centers, *rims, feat_a, feat_b, first_weight, second_weight)


def shifted(cells, axis, up):
    count = lax.axis_size(axis)
    me = lax.axis_index(axis)
    if up:
        pairs = [(i, i + 1) for i in range(count - 1)]
        edge = me == 0
    else:
        pairs = [(i + 1, i) for i in range(count - 1)]
        edge = me == count - 1
    got = lax.ppermute(cells, axis, pairs)
    return jnp.where(edge, jnp.asarray(SENT, got.dtype), got)


def exchange(centers):
    def both(rows, cols):
        return jnp.stack([center[rows, cols] for center in centers])

    near, far, all_cells = slice(0, R), slice(-R, None), slice(None)
    top = shifted(both(far, all_cells), "gy", True)
    bottom = shifted(both(near, all_cells), "gy", False)
    head, tail = (
        jnp.concatenate([top[:, :, side], both(all_cells, side), bottom[:, :, side]], axis=1)
        for side in (near, far)
    )
    left = shifted(tail, "gx", True)
    right = shifted(head, "gx", False)
    return top, bottom, left, right


def local(feat_a, feat_b, occ_a, occ_b, first_weight, second_weight):
    centers = [
        jnp.where(occ[..., None] > 0, feat, SENT).astype(jnp.bfloat16)
        for feat, occ in ((feat_a, occ_a), (feat_b, occ_b))
    ]
    feat_a, feat_b, *centers = one_pass(
        True, centers, exchange(centers), feat_a, feat_b, first_weight, second_weight
    )
    return tuple(
        one_pass(False, centers, exchange(centers), feat_a, feat_b, first_weight, second_weight)
    )


def solution(mesh):
    in_specs = (P("gy", "gx", None), P("gy", "gx", None), P("gy", "gx"), P("gy", "gx"), P(), P())
    out_specs = (P("gy", "gx", None), P("gy", "gx", None))
    return jax.shard_map(local, mesh=mesh, in_specs=in_specs, out_specs=out_specs, check_vma=False)
```

```python
import functools

import jax
import jax.numpy as jnp
from jax import lax
from jax.experimental import pallas as pl
from jax.experimental.pallas import tpu as pltpu
from jax.sharding import PartitionSpec as P


R = 8
T = 16
SENT = 2.0**120
LIMIT = 2.0**110
BIG = 2.0**100
LOG2E = 1.4426950408889634
RSQRT2 = 0.7071067811865476


def tables():
    lane = jnp.arange(128)

    def spot(shape, width):
        at = jnp.arange(width)
        row = (jnp.arange(shape[0])[:, None, None] * (width // T) + at[:, None] // T) & 31
        col = (jnp.arange(shape[1])[:, None, None] * T + at[:, None] % T) & 31
        return row[:, None], col[None]

    row, col = spot((4, 2), 128)
    inside = ((jnp.where(lane < 32, row, col) - lane) & 31) <= 2 * R
    bias = jnp.where((lane >= 64) | inside, 0.0, -BIG).astype(jnp.bfloat16)
    row, col = spot((2, 2), 256)
    hit = (lane == row) | (lane == col + 32) | (lane == 64)
    return bias, jnp.where(hit, 1.0, 0.0).astype(jnp.bfloat16)


def assemble(centers, top, bottom, left, right, corners, bias, kc, ke, vt, pc):
    sent = jnp.asarray(SENT, jnp.bfloat16)

    def group(s, rg, row_of, left_of, right_of):
        lines = [
            jnp.concatenate([left_of(r), row_of(r), right_of(r)], axis=0) for r in range(8)
        ]
        for cg in range(5):
            raw = jnp.concatenate([line[cg * T : (cg + 1) * T] for line in lines], axis=0)
            free = raw == sent
            clean = jnp.where(free, jnp.zeros_like(raw), raw)
            kc[s, rg, cg] = clean
            vt[s, rg, cg] = clean.T
            ke[s, rg, cg] = jnp.where(free, jnp.full_like(raw, -BIG), bias[rg & 3, cg & 1])

    for s in range(2):
        for rg, source, first in ((0, top, 0), (9, bottom, R)):
            group(
                s,
                rg,
                lambda r: source[s, r],
                lambda r: corners[0][s, first + r],
                lambda r: corners[1][s, first + r],
            )

    def step(rg, carry):
        row = (rg - 1) * 8
        for s in range(2):
            group(
                s,
                rg,
                lambda r: centers[s][row + r],
                lambda r: left[s, row + r],
                lambda r: right[s, row + r],
            )
        return carry

    lax.fori_loop(1, 9, step, 0)
    for s in range(2):
        for h in range(2):
            n = 768 * (1 - h)
            pc[s, n : n + 256, h * 128 : h * 128 + 128] = jnp.zeros((256, 128), jnp.bfloat16)


def kernel(
    emit, tiles, ca, cb, top, bottom, left, right, c0, c1, bias, codes, fa, fb, w1, w2, *rest
):
    keyed = (None, None)
    if emit:
        oa, ob, *rest = rest
        keyed = (rest[0], rest[1])
        rest = rest[2:]
    else:
        oa, ob, *rest = rest
    kc, ke, vt, sc, pc, ct, mx, sm = rest
    centers = (ca, cb)
    feats = (fa, fb)
    outs = (oa, ob)
    across = tiles[1]
    last = tiles[0] * tiles[1] - 1
    scale = LOG2E / 128.0**0.5
    j = pl.program_id(0)

    def place(t):
        t = jnp.clip(t, 0, last)
        return t // across, t % across

    sent = jnp.asarray(SENT, jnp.bfloat16)

    def tile_of(s, ty, tx):
        raw = centers[s][pl.ds(ty * T, T), pl.ds(pl.multiple_of(tx * T, T), T), :]
        raw = raw.reshape(256, 128)
        return raw, jnp.where(raw == sent, jnp.zeros_like(raw), raw)

    def score(s, t):
        ty, tx = place(t)
        k = 1 - s
        _, query = tile_of(s, ty, tx)
        full = jnp.concatenate([query, codes[ty & 1, tx & 1]], axis=1)
        best = [None, None]
        for i in range(2):
            rows = pl.ds(2 * ty + 2 * i, 2)
            cols = pl.ds(tx, 2)
            keys = jnp.concatenate(
                [
                    kc[k, rows, cols].reshape(512, 128),
                    ke[k, rows, cols].reshape(512, 128),
                ],
                axis=1,
            )
            scores = lax.dot_general(
                keys, full, (((1,), (1,)), ((), ())), preferred_element_type=jnp.float32
            )
            for h in range(2):
                lo, hi = max(256 * h, 512 * i), min(256 * h + 768, 512 * i + 512)
                part = scores[lo - 512 * i : hi - 512 * i, h * 128 : h * 128 + 128]
                sc[s, lo:hi, h * 128 : h * 128 + 128] = part
                top_now = part.reshape((hi - lo) // 8, 8, 128).max(0)
                best[h] = top_now if best[h] is None else jnp.maximum(best[h], top_now)
            yield
        for h in range(2):
            mx[s, :, h * 128 : h * 128 + 128] = best[h]
        yield

    def weigh(s):
        for h in range(2):
            lanes = slice(h * 128, h * 128 + 128)
            best = jnp.maximum(mx[s, :, lanes].max(0, keepdims=True), 0.0)
            total = jnp.zeros((8, 128), jnp.float32)
            for n in range(256 * h, 256 * h + 768, 128):
                e = jnp.exp2((sc[s, n : n + 128, lanes] - best) * scale)
                total = total + e.reshape(16, 8, 128).sum(0)
                pc[s, n : n + 128, lanes] = e.astype(jnp.bfloat16)
                if (n - 256 * h) % 256 == 128:
                    yield
            total = total.sum(0, keepdims=True) + jnp.exp2(-best * scale)
            sm[s, :, lanes] = jnp.broadcast_to(1.0 / total, (8, 128))
        yield

    def gather(s, t, slot):
        ty, tx = place(t)
        k = 1 - s
        values = jnp.concatenate(
            [vt[k, 2 * ty + i, tx + c] for i in range(4) for c in range(2)], axis=1
        )
        carried = jnp.dot(values, pc[s], preferred_element_type=jnp.float32)
        ct[slot] = (carried * sm[s][:1]).astype(jnp.bfloat16)
        yield

    def update(s, t, slot, side):
        ty, tx = place(t)
        raw, query = tile_of(s, ty, tx)
        joined = jnp.concatenate([query, ct[slot].T], axis=1)
        x = jnp.dot(joined, w1[...], preferred_element_type=jnp.float32)
        hidden = (x * (1.0 + lax.erf(x * RSQRT2))).astype(jnp.bfloat16)
        yield
        change = jnp.dot(hidden, w2[...], preferred_element_type=jnp.float32)
        free = raw.astype(jnp.float32) > LIMIT
        cols = slice(side * T, side * T + T)
        old = feats[s][:, cols].reshape(256, 128)
        new = jnp.where(free, old, old + change)
        outs[s][:, cols] = new.reshape(T, T, 128)
        if emit:
            next_key = jnp.where(free, SENT, new).astype(jnp.bfloat16)
            keyed[s][:, cols] = next_key.reshape(T, T, 128)
        yield

    def run(begin, end):
        for u in range(4):
            s, t = u % 2, 2 * j + u // 2
            stages = []
            if not begin:
                stages.append(update(s, t - 2, u, u // 2))
            if not (begin and u == 0) and not (end and u > 0):
                stages.append(gather(1 - s, 2 * j + (u + 1) // 2 - 1, (u + 3) % 4))
            if not end:
                stages.append(score(1 - s, 2 * j + (u + 1) // 2))
                stages.append(weigh(s))
            while stages:
                stages = [stage for stage in stages if next(stage, True) is None]

    steps = (last + 1) // 2

    @pl.when(j == 0)
    def _():
        assemble(centers, top, bottom, left, right, (c0, c1), bias, kc, ke, vt, pc)
        for unused in score(0, 0):
            pass
        run(True, False)

    @pl.when((j > 0) & (j < steps))
    def _():
        run(False, False)

    @pl.when(j == steps)
    def _():
        run(False, True)


def one_pass(emit, centers, rims, marks, feat_a, feat_b, first_weight, second_weight):
    rows, cols, channels = feat_a.shape
    tiles = (rows // T, cols // T)
    count = tiles[0] * tiles[1]
    whole = pl.BlockSpec(memory_space=pltpu.VMEM)

    def at(j):
        t = jnp.clip(2 * (j - 1), 0, count - 2)
        return t // tiles[1], (t % tiles[1]) // 2, 0

    tile = pl.BlockSpec((T, 2 * T, channels), at)
    out_shape = [jax.ShapeDtypeStruct(feat_a.shape, jnp.float32)] * 2
    out_specs = [tile, tile]
    if emit:
        out_shape += [jax.ShapeDtypeStruct(feat_a.shape, jnp.bfloat16)] * 2
        out_specs += [tile, tile]
    blocks = (2, (rows + 2 * R) // 8, (cols + 2 * R) // T, 128, 128)
    flops = 2 * 16 * (2 * 1024 * 256 * 256 * 2 + 256 * 256 * 384 * 2)
    return pl.pallas_call(
        functools.partial(kernel, emit, tiles),
        grid=(count // 2 + 1,),
        in_specs=[whole] * 10 + [tile, tile, whole, whole],
        out_specs=out_specs,
        out_shape=out_shape,
        scratch_shapes=[
            pltpu.VMEM(blocks, jnp.bfloat16),
            pltpu.VMEM(blocks, jnp.bfloat16),
            pltpu.VMEM(blocks, jnp.bfloat16),
            pltpu.VMEM((2, 1024, 256), jnp.float32),
            pltpu.VMEM((2, 1024, 256), jnp.bfloat16),
            pltpu.VMEM((4, 128, 256), jnp.bfloat16),
            pltpu.VMEM((2, 8, 256), jnp.float32),
            pltpu.VMEM((2, 8, 256), jnp.float32),
        ],
        compiler_params=pltpu.CompilerParams(
            dimension_semantics=("arbitrary",), vmem_limit_bytes=44 << 20
        ),
        cost_estimate=pl.CostEstimate(
            flops=flops, bytes_accessed=14 << 20, transcendentals=2 * 16 * 768 * 256
        ),
        name="match_pass",
    )(*centers, *rims, *marks, feat_a, feat_b, first_weight, second_weight)


def shifted(cells, axis, up):
    count = lax.axis_size(axis)
    me = lax.axis_index(axis)
    if up:
        pairs = [(i, i + 1) for i in range(count - 1)]
        edge = me == 0
    else:
        pairs = [(i + 1, i) for i in range(count - 1)]
        edge = me == count - 1
    got = lax.ppermute(cells, axis, pairs)
    return jnp.where(edge, jnp.asarray(SENT, got.dtype), got)


def exchange(centers):
    def both(rows, cols):
        return jnp.stack([center[rows, cols] for center in centers])

    near, far, all_cells = slice(0, R), slice(-R, None), slice(None)
    top = shifted(both(far, all_cells), "gy", True)
    bottom = shifted(both(near, all_cells), "gy", False)
    left = shifted(both(all_cells, far), "gx", True)
    right = shifted(both(all_cells, near), "gx", False)
    head, tail = (
        jnp.concatenate([top[:, :, side], bottom[:, :, side]], axis=1) for side in (near, far)
    )
    return top, bottom, left, right, shifted(tail, "gx", True), shifted(head, "gx", False)


def local(feat_a, feat_b, occ_a, occ_b, first_weight, second_weight):
    centers = [
        jnp.where(occ[..., None] > 0, feat, SENT).astype(jnp.bfloat16)
        for feat, occ in ((feat_a, occ_a), (feat_b, occ_b))
    ]
    marks = tables()
    weights = (first_weight, second_weight * jnp.asarray(0.5, second_weight.dtype))
    rims = exchange(centers)
    feat_a, feat_b, *centers = one_pass(True, centers, rims, marks, feat_a, feat_b, *weights)
    rims = exchange(centers)
    return tuple(one_pass(False, centers, rims, marks, feat_a, feat_b, *weights))


def solution(mesh):
    in_specs = (P("gy", "gx", None), P("gy", "gx", None), P("gy", "gx"), P("gy", "gx"), P(), P())
    out_specs = (P("gy", "gx", None), P("gy", "gx", None))
    return jax.shard_map(local, mesh=mesh, in_specs=in_specs, out_specs=out_specs, check_vma=False)
```

```python
import functools

import jax
import jax.numpy as jnp
from jax import lax
from jax.experimental import pallas as pl
from jax.experimental.pallas import tpu as pltpu
from jax.sharding import PartitionSpec as P


R = 8
T = 16
SENT = 2.0**120
LIMIT = 2.0**110
BIG = 2.0**100
LOG2E = 1.4426950408889634
RSQRT2 = 0.7071067811865476


def tables():
    lane = jnp.arange(128)

    def spot(shape, width):
        at = jnp.arange(width)
        row = (jnp.arange(shape[0])[:, None, None] * (width // T) + at[:, None] // T) & 31
        col = (jnp.arange(shape[1])[:, None, None] * T + at[:, None] % T) & 31
        return row[:, None], col[None]

    row, col = spot((4, 2), 128)
    inside = ((jnp.where(lane < 32, row, col) - lane) & 31) <= 2 * R
    bias = jnp.where((lane >= 64) | inside, 0.0, -BIG).astype(jnp.bfloat16)
    row, col = spot((2, 2), 256)
    hit = (lane == row) | (lane == col + 32) | (lane == 64)
    return bias, jnp.where(hit, 1.0, 0.0).astype(jnp.bfloat16)


def assemble(centers, top, bottom, left, right, bias, kc, ke, vt, pc):
    sent = jnp.asarray(SENT, jnp.bfloat16)

    def group(s, rg, lines):
        for cg in range(5):
            raw = jnp.concatenate([line[cg * T : (cg + 1) * T] for line in lines], axis=0)
            free = raw == sent
            clean = jnp.where(free, jnp.zeros_like(raw), raw)
            kc[s, rg, cg] = clean
            vt[s, rg, cg] = clean.T
            ke[s, rg, cg] = jnp.where(free, jnp.full_like(raw, -BIG), bias[rg & 3, cg & 1])

    for s in range(2):
        for rg, source in ((0, top), (9, bottom)):
            group(s, rg, [source[s, r] for r in range(8)])

    def step(rg, carry):
        row = (rg - 1) * 8
        for s in range(2):
            lines = [
                jnp.concatenate(
                    [left[s, row + r], centers[s][row + r], right[s, row + r]], axis=0
                )
                for r in range(8)
            ]
            group(s, rg, lines)
        return carry

    lax.fori_loop(1, 9, step, 0)
    for s in range(2):
        for h in range(2):
            n = 768 * (1 - h)
            pc[s, n : n + 256, h * 128 : h * 128 + 128] = jnp.zeros((256, 128), jnp.bfloat16)


def kernel(
    emit, tiles, ca, cb, top, bottom, left, right, bias, codes, fa, fb, w1, w2, *rest
):
    keyed = (None, None)
    if emit:
        oa, ob, *rest = rest
        keyed = (rest[0], rest[1])
        rest = rest[2:]
    else:
        oa, ob, *rest = rest
    kc, ke, vt, sc, pc, ct, mx, sm = rest
    centers = (ca, cb)
    feats = (fa, fb)
    outs = (oa, ob)
    across = tiles[1]
    last = tiles[0] * tiles[1] - 1
    scale = LOG2E / 128.0**0.5
    j = pl.program_id(0)

    def place(t):
        t = jnp.clip(t, 0, last)
        return t // across, t % across

    sent = jnp.asarray(SENT, jnp.bfloat16)

    def tile_of(s, ty, tx):
        raw = centers[s][pl.ds(ty * T, T), pl.ds(pl.multiple_of(tx * T, T), T), :]
        raw = raw.reshape(256, 128)
        return raw, jnp.where(raw == sent, jnp.zeros_like(raw), raw)

    def score(s, t):
        ty, tx = place(t)
        k = 1 - s
        _, query = tile_of(s, ty, tx)
        full = jnp.concatenate([query, codes[ty & 1, tx & 1]], axis=1)
        best = [None, None]
        for i in range(2):
            rows = pl.ds(2 * ty + 2 * i, 2)
            cols = pl.ds(tx, 2)
            keys = jnp.concatenate(
                [
                    kc[k, rows, cols].reshape(512, 128),
                    ke[k, rows, cols].reshape(512, 128),
                ],
                axis=1,
            )
            scores = lax.dot_general(
                keys, full, (((1,), (1,)), ((), ())), preferred_element_type=jnp.float32
            )
            for h in range(2):
                lo, hi = max(256 * h, 512 * i), min(256 * h + 768, 512 * i + 512)
                part = scores[lo - 512 * i : hi - 512 * i, h * 128 : h * 128 + 128]
                sc[s, lo:hi, h * 128 : h * 128 + 128] = part
                top_now = part.reshape((hi - lo) // 8, 8, 128).max(0)
                best[h] = top_now if best[h] is None else jnp.maximum(best[h], top_now)
            yield
        for h in range(2):
            mx[s, :, h * 128 : h * 128 + 128] = best[h]
        yield

    def weigh(s):
        for h in range(2):
            lanes = slice(h * 128, h * 128 + 128)
            best = jnp.maximum(mx[s, :, lanes].max(0, keepdims=True), 0.0)
            total = jnp.zeros((8, 128), jnp.float32)
            for n in range(256 * h, 256 * h + 768, 128):
                e = jnp.exp2((sc[s, n : n + 128, lanes] - best) * scale)
                total = total + e.reshape(16, 8, 128).sum(0)
                pc[s, n : n + 128, lanes] = e.astype(jnp.bfloat16)
                if (n - 256 * h) % 256 == 128:
                    yield
            total = total.sum(0, keepdims=True) + jnp.exp2(-best * scale)
            sm[s, :, lanes] = jnp.broadcast_to(1.0 / total, (8, 128))
        yield

    def gather(s, t, slot):
        ty, tx = place(t)
        k = 1 - s
        values = jnp.concatenate(
            [vt[k, 2 * ty + i, tx + c] for i in range(4) for c in range(2)], axis=1
        )
        carried = jnp.dot(values, pc[s], preferred_element_type=jnp.float32)
        ct[slot] = (carried * sm[s][:1]).astype(jnp.bfloat16)
        yield

    def update(s, t, slot, side):
        ty, tx = place(t)
        raw, query = tile_of(s, ty, tx)
        joined = jnp.concatenate([query, ct[slot].T], axis=1)
        x = jnp.dot(joined, w1[...], preferred_element_type=jnp.float32)
        hidden = (x * (1.0 + lax.erf(x * RSQRT2))).astype(jnp.bfloat16)
        yield
        change = jnp.dot(hidden, w2[...], preferred_element_type=jnp.float32)
        free = raw.astype(jnp.float32) > LIMIT
        cols = slice(side * T, side * T + T)
        old = feats[s][:, cols].reshape(256, 128)
        new = jnp.where(free, old, old + change)
        outs[s][:, cols] = new.reshape(T, T, 128)
        if emit:
            next_key = jnp.where(free, SENT, new).astype(jnp.bfloat16)
            keyed[s][:, cols] = next_key.reshape(T, T, 128)
        yield

    def run(begin, end):
        for u in range(4):
            s, t = u % 2, 2 * j + u // 2
            stages = []
            if not begin:
                stages.append(update(s, t - 2, u, u // 2))
            if not (begin and u == 0) and not (end and u > 0):
                stages.append(gather(1 - s, 2 * j + (u + 1) // 2 - 1, (u + 3) % 4))
            if not end:
                stages.append(score(1 - s, 2 * j + (u + 1) // 2))
                stages.append(weigh(s))
            while stages:
                stages = [stage for stage in stages if next(stage, True) is None]

    steps = (last + 1) // 2

    @pl.when(j == 0)
    def _():
        assemble(centers, top, bottom, left, right, bias, kc, ke, vt, pc)
        for unused in score(0, 0):
            pass
        run(True, False)

    @pl.when((j > 0) & (j < steps))
    def _():
        run(False, False)

    @pl.when(j == steps)
    def _():
        run(False, True)


def one_pass(emit, centers, rims, marks, feat_a, feat_b, first_weight, second_weight):
    rows, cols, channels = feat_a.shape
    tiles = (rows // T, cols // T)
    count = tiles[0] * tiles[1]
    whole = pl.BlockSpec(memory_space=pltpu.VMEM)

    def at(j):
        t = jnp.clip(2 * (j - 1), 0, count - 2)
        return t // tiles[1], (t % tiles[1]) // 2, 0

    tile = pl.BlockSpec((T, 2 * T, channels), at)
    out_shape = [jax.ShapeDtypeStruct(feat_a.shape, jnp.float32)] * 2
    out_specs = [tile, tile]
    if emit:
        out_shape += [jax.ShapeDtypeStruct(feat_a.shape, jnp.bfloat16)] * 2
        out_specs += [tile, tile]
    blocks = (2, (rows + 2 * R) // 8, (cols + 2 * R) // T, 128, 128)
    flops = 2 * 16 * (2 * 1024 * 256 * 256 * 2 + 256 * 256 * 384 * 2)
    return pl.pallas_call(
        functools.partial(kernel, emit, tiles),
        grid=(count // 2 + 1,),
        in_specs=[whole] * 8 + [tile, tile, whole, whole],
        out_specs=out_specs,
        out_shape=out_shape,
        scratch_shapes=[
            pltpu.VMEM(blocks, jnp.bfloat16),
            pltpu.VMEM(blocks, jnp.bfloat16),
            pltpu.VMEM(blocks, jnp.bfloat16),
            pltpu.VMEM((2, 1024, 256), jnp.float32),
            pltpu.VMEM((2, 1024, 256), jnp.bfloat16),
            pltpu.VMEM((4, 128, 256), jnp.bfloat16),
            pltpu.VMEM((2, 8, 256), jnp.float32),
            pltpu.VMEM((2, 8, 256), jnp.float32),
        ],
        compiler_params=pltpu.CompilerParams(
            dimension_semantics=("arbitrary",), vmem_limit_bytes=44 << 20
        ),
        cost_estimate=pl.CostEstimate(
            flops=flops, bytes_accessed=14 << 20, transcendentals=2 * 16 * 768 * 256
        ),
        name="match_pass",
    )(*centers, *rims, *marks, feat_a, feat_b, first_weight, second_weight)


def shifted(cells, axis, up):
    count = lax.axis_size(axis)
    me = lax.axis_index(axis)
    if up:
        pairs = [(i, i + 1) for i in range(count - 1)]
        edge = me == 0
    else:
        pairs = [(i + 1, i) for i in range(count - 1)]
        edge = me == count - 1
    got = lax.ppermute(cells, axis, pairs)
    return jnp.where(edge, jnp.asarray(SENT, got.dtype), got)


def exchange(centers):
    def both(rows, cols):
        return jnp.stack([center[rows, cols] for center in centers])

    near, far, all_cells = slice(0, R), slice(-R, None), slice(None)

    def ends(cols):
        return jnp.concatenate([both(near, cols), both(far, cols)], axis=1)

    west = shifted(ends(far), "gx", True)
    east = shifted(ends(near), "gx", False)
    left = shifted(both(all_cells, far), "gx", True)
    right = shifted(both(all_cells, near), "gx", False)

    def wide(rows):
        return jnp.concatenate([west[:, rows], both(rows, all_cells), east[:, rows]], axis=2)

    top = shifted(wide(far), "gy", True)
    bottom = shifted(wide(near), "gy", False)
    return top, bottom, left, right


def local(feat_a, feat_b, occ_a, occ_b, first_weight, second_weight):
    centers = [
        jnp.where(occ[..., None] > 0, feat, SENT).astype(jnp.bfloat16)
        for feat, occ in ((feat_a, occ_a), (feat_b, occ_b))
    ]
    marks = tables()
    weights = (first_weight, second_weight * jnp.asarray(0.5, second_weight.dtype))
    rims = exchange(centers)
    feat_a, feat_b, *centers = one_pass(True, centers, rims, marks, feat_a, feat_b, *weights)
    rims = exchange(centers)
    return tuple(one_pass(False, centers, rims, marks, feat_a, feat_b, *weights))


def solution(mesh):
    in_specs = (P("gy", "gx", None), P("gy", "gx", None), P("gy", "gx"), P("gy", "gx"), P(), P())
    out_specs = (P("gy", "gx", None), P("gy", "gx", None))
    return jax.shard_map(local, mesh=mesh, in_specs=in_specs, out_specs=out_specs, check_vma=False)
```
